32 devices in a mesh: row: 4 (over z), col: 4 (over x, core), depth: 2 (over y).
Axes of the slice: x: 2, y: 2, z: 4, core: 2. Of those that a mesh axis runs over, the one named last changes fastest.
Arguments:
- tokens: bfloat16 [2048, 8192], P(('row', 'col'), 'depth'), may hold values from -0.3125 to 0.3125
- weight: bfloat16 [8192, 8192], P('depth', ('col', 'row')), may hold values from -0.0625 to 0.0625
- grad_output: bfloat16 [2048, 8192], P('row', ('col', 'depth')), may hold values from -6 to 6
Outputs:
- grad_input: bfloat16 [2048, 8192], P(('row', 'col'), 'depth')
- grad_weight: bfloat16 [8192, 8192], P('depth', ('col', 'row'))
The draws below stay inside these ranges and needn't reach their ends.
All inputs are finite; a program needn't handle non-finite values.
Results may differ from the reference program's by a relative error of at most 0.001.
Values may be sent and summed in bfloat16 or wider, within the bound.
No kernel may reach another device: no remote copies, remote signals or barrier semaphores. Data moves between devices by JAX's collectives and lax.ppermute only.
A program may use at most 128 MiB of HBM per device.

```python
import jax
import jax.numpy as jnp

D_IN = 8192
D_OUT = 8192
TOKENS = 2048


def spiked(drawn, stream_key, source, target, parts, factor):
    def block_of(axis_at):
        return (jnp.arange(drawn.shape[axis_at]) // (drawn.shape[axis_at] // parts)).reshape((-1,) + (1,) * (drawn.ndim - 1 - axis_at))

    one_side = jax.random.permutation(stream_key, parts)[block_of(target)]
    other_side = (block_of(target) + parts // 2) % parts
    return jnp.where((block_of(source) == one_side) | (block_of(source) == other_side), factor * drawn, drawn)


def shard_levels(rng, extent, pieces, low, top_value):
    gain, own = 1.0, jax.random.fold_in(rng, 6)
    for position, shards_of in pieces:
        steps = jnp.exp(jax.random.uniform(jax.random.fold_in(own, position), (shards_of,), jnp.float32, low / len(pieces), top_value / len(pieces)))
        gain = gain * jnp.repeat(steps, extent[position] // shards_of).reshape([-1 if axis == position else 1 for axis in range(len(extent))])
    return gain


def bell_draw(rng, dims, width, reach, pieces=(), kind=jnp.bfloat16):
    factor_of = shard_levels(rng, dims, pieces, -0.22, 0.18) if pieces else 1.0
    result = jax.random.normal(rng, dims, jnp.float32) * width * factor_of
    return jnp.minimum(jnp.maximum(result, -reach), reach).astype(kind)


def bell_draw_with(stream_key, shape, width, most, pieces, heavy, held_as=jnp.bfloat16):
    drawn = width * jax.random.normal(stream_key, shape, jnp.float32)
    if pieces:
        drawn = drawn * shard_levels(stream_key, shape, pieces, -0.22, 0.18)
    return jnp.clip(spiked(drawn, jax.random.fold_in(stream_key, 3), *heavy), -most, most).astype(held_as)


def setup_inputs(seed: int = 0) -> dict:
    keys = jax.random.split(jax.random.key(seed), 4)
    tokens = bell_draw(keys[0], (TOKENS, D_IN), (TOKENS ** -0.5), 0.3125, ((0, 16), (1, 2)))
    weight = bell_draw(keys[1], (D_IN, D_OUT), D_IN ** -0.5, 0.0625, ((0, 2), (1, 16)))
    grad_output = bell_draw_with(keys[2], (TOKENS, D_OUT), 1.0, 6.0, ((0, 4), (1, 8)), (1, 0, 8, 2.0))
    return {"tokens": tokens, "weight": weight, "grad_output": grad_output}


def reference(tokens, weight, grad_output):
    grad_input = jnp.dot(grad_output, weight.T, preferred_element_type=jnp.float32).astype(jnp.bfloat16)
    grad_weight = jnp.dot(tokens.T, grad_output, preferred_element_type=jnp.float32).astype(jnp.bfloat16)
    return grad_input, grad_weight
```

```python
import functools

import jax
import jax.numpy as jnp
from jax import lax
from jax.experimental import pallas as pl
from jax.experimental.pallas import tpu as pltpu
from jax.sharding import PartitionSpec as P


BF16 = jnp.bfloat16
F32 = jnp.float32
last_with_last = (((1,), (1,)), ((), ()))
first_with_first = (((0,), (0,)), ((), ()))
PAD = 16
TILE = 64
LIFT = 7.5
CHUNKS = 1


def flip(value, axis, bit, size):
    return lax.ppermute(value, axis, [(i, i ^ bit) for i in range(size)])


def swap_pieces(piece_for, size):
    got = {d: flip(piece_for(d), "col", d, size) for d in sorted(range(1, size), reverse=True)}
    got[0] = piece_for(0)
    return [got[d] for d in range(size)]


def gather_line(mine, size):
    up, down = [mine], [mine]
    for s in range(1, size):
        up.append(lax.ppermute(up[-1], "row", [(i, i + 1) for i in range(s - 1, size - 1)]))
        down.append(lax.ppermute(down[-1], "row", [(i, i - 1) for i in range(1, size - s + 1)]))
    me = lax.axis_index("row")
    return [mine] + [jnp.where(me >= j, up[j], down[size - j]) for j in range(1, size)]


def unpacked(ref, rows, tile):
    scale = ref[pl.ds(ref.shape[0] - PAD, 8), :].astype(F32)[:1] - LIFT
    coded = ref[pl.ds(rows, tile), :].astype(F32)
    size = jnp.exp2(jnp.log2(jnp.abs(coded)) * 0.0625 + scale)
    return jnp.where(coded < 0, -size, size)


def encode(term, came, out, total):
    size, width = total.shape

    def add(t, top):
        rows = pl.multiple_of(t * TILE, TILE)
        value = term[pl.ds(rows, TILE), :]
        if came is not None:
            value = value + unpacked(came, rows, TILE)
        total[pl.ds(rows, TILE), :] = value
        return jnp.maximum(top, jnp.max(jnp.abs(value), axis=0, keepdims=True))

    top = lax.fori_loop(0, size // TILE, add, jnp.full((1, width), 1e-30, F32))
    power = jnp.floor(jnp.log2(jnp.max(top, axis=1, keepdims=True))) + 1.0
    scale = jnp.exp2(LIFT - power)

    def code(t, carry):
        rows = pl.multiple_of(t * TILE, TILE)
        value = total[pl.ds(rows, TILE), :]
        unit = value * scale
        unit = unit * unit
        unit = unit * unit
        unit = unit * unit
        unit = unit * unit
        out[pl.ds(rows, TILE), :] = jnp.where(value < 0, -unit, unit).astype(BF16)
        return carry

    lax.fori_loop(0, size // TILE, code, 0)
    out[pl.ds(size, PAD), :] = jnp.broadcast_to(power, (PAD, width)).astype(BF16)


def pack_first(term, out, total):
    encode(term, None, out, total)


def pack_sum(term, came, out, total):
    encode(term, came, out, total)


def pack_or_copy(at_end, other, term, came, out, total):
    @pl.when(at_end[0] == 1)
    def _():
        out[...] = other[...]

    @pl.when(at_end[0] != 1)
    def _():
        encode(term, came, out, total)


def in_vmem(count):
    return [pl.BlockSpec(memory_space=pltpu.VMEM)] * count


def pack(term, came=None, at_end=None, other=None):
    size, width = term.shape
    call = functools.partial(
        pl.pallas_call,
        out_shape=jax.ShapeDtypeStruct((size + PAD, width), BF16),
        out_specs=in_vmem(1)[0],
        scratch_shapes=[pltpu.VMEM((size, width), F32)],
        cost_estimate=pl.CostEstimate(
            flops=size * width * 4000, bytes_accessed=size * width * 8, transcendentals=0
        ),
    )
    if came is None:
        return call(pack_first, in_specs=in_vmem(1))(term)
    if other is None:
        return call(pack_sum, in_specs=in_vmem(2))(term, came)
    flag = pl.BlockSpec(memory_space=pltpu.SMEM)
    return call(pack_or_copy, in_specs=[flag] + in_vmem(3))(at_end, other, term, came)


def finish_kernel(term, one, two, out):
    def body(t, carry):
        rows = pl.multiple_of(t * TILE, TILE)
        value = term[pl.ds(rows, TILE), :] + unpacked(one, rows, TILE) + unpacked(two, rows, TILE)
        out[pl.ds(rows, TILE), :] = value.astype(BF16)
        return carry

    lax.fori_loop(0, term.shape[0] // TILE, body, 0)


def finish(term, one, two):
    size, width = term.shape
    return pl.pallas_call(
        finish_kernel,
        in_specs=in_vmem(3),
        out_specs=in_vmem(1)[0],
        out_shape=jax.ShapeDtypeStruct((size, width), BF16),
        cost_estimate=pl.CostEstimate(
            flops=size * width * 4000, bytes_accessed=size * width * 10, transcendentals=0
        ),
    )(term, one, two)


def terms_kernel(cols, swap, *refs):
    pieces, weights, outs = refs[: 2 * cols], refs[2 * cols : 3 * cols], refs[3 * cols :]
    half = pieces[0].shape[1]
    mine = weights[0].shape[0]
    tile, wide = min(half, 256), min(mine, 256)

    def body(n, carry):
        at = pl.multiple_of(n * wide, wide)
        for i in range(2):
            entry = i ^ swap[0]
            for e in range(2):
                for m in range(half // tile):
                    total = None
                    for d in range(cols):
                        one = lax.dot_general(
                            pieces[2 * d + e][entry, pl.ds(m * tile, tile), :],
                            weights[d][pl.ds(at, wide), :],
                            last_with_last,
                            preferred_element_type=F32,
                        )
                        total = one if total is None else total + one
                    outs[i][pl.ds(e * half + m * tile, tile), pl.ds(at, wide)] = total
        return carry

    lax.fori_loop(0, mine // wide, body, 0)


def input_terms(pieces, weights, swap):
    cols = len(weights)
    half, width = pieces[0, 0].shape[1:]
    mine = weights[0].shape[0]
    term = jax.ShapeDtypeStruct((2 * half, mine), F32)
    return pl.pallas_call(
        functools.partial(terms_kernel, cols),
        in_specs=[pl.BlockSpec(memory_space=pltpu.SMEM)] + in_vmem(3 * cols),
        out_specs=tuple(in_vmem(2)),
        out_shape=(term, term),
        cost_estimate=pl.CostEstimate(
            flops=8 * half * mine * cols * width,
            bytes_accessed=2 * (4 * half + mine) * cols * width + 16 * half * mine,
            transcendentals=0,
        ),
    )(swap, *[pieces[d, e] for d in range(cols) for e in range(2)], *weights)


def reduce_line(near, far):
    z = lax.axis_index("row")
    at_end = jnp.where((z == 0) | (z == 3), 1, 0).astype(jnp.int32).reshape(1)
    outer, inner = near()
    came = lax.ppermute(pack(outer), "row", [(0, 1), (3, 2)])
    two, own = far()
    message = pack(two, came)
    from_end = lax.ppermute(message, "row", [(0, 1), (3, 2)])
    from_middle = lax.ppermute(message, "row", [(1, 2), (2, 1)])
    inward = pack(inner, from_end)
    one = lax.ppermute(inward, "row", [(1, 2), (2, 1)])
    mixed = pack(outer, from_middle, at_end, inward)
    other = lax.ppermute(mixed, "row", [(0, 1), (3, 2), (1, 0), (2, 3)])
    return finish(own, one, other)


def spread_grad(grad, groups, rows, cols):
    z, y = lax.axis_index("row"), lax.axis_index("depth")
    half = grad.shape[0] // 2
    per = rows // 2
    width = grad.shape[1] // per
    other = lax.dynamic_slice_in_dim(grad, (1 - y) * half, half, 0)
    own = lax.dynamic_slice_in_dim(grad, y * half, half, 0)
    came = flip(other, "depth", 1, 2)

    def piece(j):
        to = lax.rem(z + j, rows)
        both = jnp.where(lax.div(to, per) == y, own, came)
        block = lax.dynamic_slice_in_dim(both, lax.rem(to, per) * width, width, 1)
        if not j:
            return block
        return lax.ppermute(block, "row", [(i, (i + j) % rows) for i in range(rows)])

    pieces = {j: piece(j) for group in groups for j in group}
    out = []
    bits = [1 << b for b in range(cols.bit_length() - 1)]
    for group in groups:
        have = {(0, 0): jnp.stack([pieces[j] for j in group])}
        for bit in reversed(bits[1:]):
            have.update({(d ^ bit, e): flip(v, "col", bit, cols) for (d, e), v in have.items()})
        have.update({(d, 1): flip(v, "depth", 1, 2) for (d, e), v in have.items()})
        for bit in bits[:1]:
            have.update({(d ^ bit, e): flip(v, "col", bit, cols) for (d, e), v in have.items()})
        out.append(have)
    return out


def per_device(rows, cols, tokens, weight, grad_output):
    z, q, y = lax.axis_index("row"), lax.axis_index("col"), lax.axis_index("depth")
    features, outs = weight.shape
    mine = features // cols
    few = tokens.shape[0]
    block_rows = few * cols
    half = block_rows // 2
    part = mine // CHUNKS

    def token_piece(d):
        return lax.dynamic_slice_in_dim(tokens, (q ^ d) * mine, mine, 1)

    def row_start(d):
        return lax.rem((q ^ d) * few + y * half, block_rows)

    block = jnp.zeros((block_rows, mine), tokens.dtype)
    for d, piece in enumerate(swap_pieces(token_piece, cols)):
        block = lax.dynamic_update_slice_in_dim(block, piece, row_start(d), 0)

    weights = []
    for h in range(CHUNKS):

        def weight_piece(d):
            return lax.dynamic_slice_in_dim(weight, (q ^ d) * mine + h * part, part, 0)

        weights.append(swap_pieces(weight_piece, cols))

    groups = [(1, 3), (2, 0)]
    spread = spread_grad(grad_output, groups, rows, cols)
    token_slots = gather_line(block, rows)

    lower = jnp.where(z < 2, 0, 1).astype(jnp.int32).reshape(1)
    straight = jnp.zeros((1,), jnp.int32)
    grad_input = jnp.zeros((few, features), BF16)
    for h in range(CHUNKS):
        summed = reduce_line(
            lambda: input_terms(spread[0], weights[h], lower), lambda: input_terms(spread[1], weights[h], straight)
        )

        def input_piece(d):
            return lax.dynamic_slice_in_dim(summed, row_start(d), few, 0)

        for d, piece in enumerate(swap_pieces(input_piece, cols)):
            grad_input = lax.dynamic_update_slice_in_dim(
                grad_input, piece, (q ^ d) * mine + h * part, 1
            )

    all_tokens = jnp.concatenate(
        [token_slots[j][e * half : (e + 1) * half] for g in groups for e in range(2) for j in g]
    )

    def gradient_piece(d):
        piece = jnp.concatenate([spread[g][d, e].reshape(-1, outs) for g in range(2) for e in range(2)])
        return lax.dot_general(
            all_tokens, piece, first_with_first, preferred_element_type=F32
        ).astype(BF16)

    grad_weight = jnp.zeros((features, outs), BF16)
    for d, piece in enumerate(swap_pieces(gradient_piece, cols)):
        grad_weight = lax.dynamic_update_slice_in_dim(grad_weight, piece, (q ^ d) * mine, 0)
    return grad_input, grad_weight


def solution(mesh):
    rows, cols = mesh.shape["row"], mesh.shape["col"]

    def body(tokens, weight, grad_output):
        return per_device(rows, cols, tokens, weight, grad_output)

    return jax.shard_map(
        body,
        mesh=mesh,
        in_specs=(
            P(("row", "col"), "depth"),
            P("depth", ("col", "row")),
            P("row", ("col", "depth")),
        ),
        out_specs=(P(("row", "col"), "depth"), P("depth", ("col", "row"))),
        check_vma=False,
    )
```

```python
import functools

import jax
import jax.numpy as jnp
from jax import lax
from jax.experimental import pallas as pl
from jax.experimental.pallas import tpu as pltpu
from jax.sharding import PartitionSpec as P


BF16 = jnp.bfloat16
F32 = jnp.float32
last_with_last = (((1,), (1,)), ((), ()))
first_with_first = (((0,), (0,)), ((), ()))
PAD = 16
GRANT = 20 * 2**20
TILE = 64
LIFT = 7.5
CHUNKS = 1


def flip(value, axis, bit, size):
    return lax.ppermute(value, axis, [(i, i ^ bit) for i in range(size)])


def swap_pieces(piece_for, size):
    got = {d: flip(piece_for(d), "col", d, size) for d in sorted(range(1, size), reverse=True)}
    got[0] = piece_for(0)
    return [got[d] for d in range(size)]


def gather_line(mine, size):
    up, down = [mine], [mine]
    for s in range(1, size):
        up.append(lax.ppermute(up[-1], "row", [(i, i + 1) for i in range(s - 1, size - 1)]))
        down.append(lax.ppermute(down[-1], "row", [(i, i - 1) for i in range(1, size - s + 1)]))
    me = lax.axis_index("row")
    return [mine] + [jnp.where(me >= j, up[j], down[size - j]) for j in range(1, size)]


def unpacked(ref, rows, cols):
    scale = ref[pl.ds(ref.shape[0] - PAD, 8), cols].astype(F32)[:1] - LIFT
    coded = ref[rows, cols].astype(F32)
    size = jnp.exp2(jnp.log2(jnp.abs(coded)) * 0.0625 + scale)
    return jnp.where(coded < 0, -size, size)


def parts_of(terms, came):
    at = 0
    for i, term in enumerate(terms):
        width = term.shape[1]
        mine = pl.ds(at, width)
        if not came:
            yield mine, term, None, None
        elif len(came) == len(terms):
            yield mine, term, came[i], pl.ds(0, width)
        else:
            yield mine, term, came[0], mine
        at += width


def encode(terms, came, out, total):
    size, width = total.shape

    def add(t, tops):
        rows = pl.ds(pl.multiple_of(t * TILE, TILE), TILE)
        after = []
        for top, (mine, term, message, cols) in zip(tops, parts_of(terms, came)):
            value = term[rows, :]
            if message is not None:
                value = value + unpacked(message, rows, cols)
            total[rows, mine] = value
            after.append(jnp.maximum(top, jnp.max(jnp.abs(value), axis=0, keepdims=True)))
        return tuple(after)

    low = tuple(jnp.full((1, term.shape[1]), 1e-30, F32) for term in terms)
    tops = lax.fori_loop(0, size // TILE, add, low)
    top = functools.reduce(jnp.maximum, [jnp.max(t, axis=1, keepdims=True) for t in tops])
    power = jnp.floor(jnp.log2(top)) + 1.0
    scale = jnp.exp2(LIFT - power)

    def code(t, carry):
        rows = pl.ds(pl.multiple_of(t * TILE, TILE), TILE)
        value = total[rows, :]
        unit = value * scale
        unit = unit * unit
        unit = unit * unit
        unit = unit * unit
        unit = unit * unit
        out[rows, :] = jnp.where(value < 0, -unit, unit).astype(BF16)
        return carry

    lax.fori_loop(0, size // TILE, code, 0)
    out[pl.ds(size, PAD), :] = jnp.broadcast_to(power, (PAD, width)).astype(BF16)


def pack_kernel(count, at_end, *refs):
    refs = list(refs)
    total, out = refs.pop(), refs.pop()
    terms, came = refs[:count], refs[count:]
    if at_end is None:
        encode(terms, came, out, total)
        return
    other = came.pop()

    @pl.when(at_end[0] == 1)
    def _():
        out[...] = other[...]

    @pl.when(at_end[0] != 1)
    def _():
        encode(terms, came, out, total)


def in_vmem(count):
    return [pl.BlockSpec(memory_space=pltpu.VMEM)] * count


def pack(terms, came=(), at_end=None, other=None):
    size, width = terms[0].shape[0], sum(term.shape[1] for term in terms)
    operands = [*terms, *came]
    specs = in_vmem(len(operands))
    kernel = functools.partial(pack_kernel, len(terms), None)
    if other is not None:
        operands = [at_end, *operands, other]
        specs = [pl.BlockSpec(memory_space=pltpu.SMEM)] + specs + in_vmem(1)
        kernel = functools.partial(pack_kernel, len(terms))
    return pl.pallas_call(
        kernel,
        in_specs=specs,
        out_specs=in_vmem(1)[0],
        out_shape=jax.ShapeDtypeStruct((size + PAD, width), BF16),
        scratch_shapes=[pltpu.VMEM((size, width), F32)],
        compiler_params=pltpu.CompilerParams(vmem_limit_bytes=GRANT),
        cost_estimate=pl.CostEstimate(
            flops=size * width * 4000, bytes_accessed=size * width * 8, transcendentals=0
        ),
    )(*operands)


def finish_kernel(count, starts, *refs):
    terms, (one, two), outs = refs[:count], refs[count : count + 2], refs[count + 2 :]
    tile = min(TILE, outs[0].shape[0])
    for i, out in enumerate(outs):
        for t in range(out.shape[0] // tile):
            rows = pl.ds(pl.multiple_of(starts[i] + t * tile, tile), tile)
            for mine, term, message, cols in parts_of(terms, [one]):
                value = term[rows, :] + unpacked(one, rows, cols) + unpacked(two, rows, cols)
                out[pl.ds(t * tile, tile), mine] = value.astype(BF16)


def finish(terms, one, two, starts, rows):
    width, count = one.shape[1], len(terms)
    call = pl.pallas_call(
        functools.partial(finish_kernel, count),
        in_specs=[pl.BlockSpec(memory_space=pltpu.SMEM)] + in_vmem(count + 2),
        out_specs=tuple(in_vmem(len(starts))),
        out_shape=(jax.ShapeDtypeStruct((rows, width), BF16),) * len(starts),
        compiler_params=pltpu.CompilerParams(vmem_limit_bytes=GRANT),
        cost_estimate=pl.CostEstimate(
            flops=rows * len(starts) * width * 4000,
            bytes_accessed=rows * len(starts) * width * 10,
            transcendentals=0,
        ),
    )
    return list(call(jnp.stack(starts).astype(jnp.int32), *terms, one, two))


def terms_kernel(cols, which, *refs):
    pieces, refs = refs[: 2 * cols], refs[2 * cols :]
    chunks = len(refs) // (cols + 1)
    half = pieces[0].shape[1]
    entry = which[0]
    tile = min(half, 256)
    for c in range(chunks):
        weights, out = refs[c * cols : (c + 1) * cols], refs[chunks * cols + c]
        mine = weights[0].shape[0]
        wide = min(mine, 256)

        def body(n, carry):
            at = pl.multiple_of(n * wide, wide)
            for e in range(2):
                for m in range(half // tile):
                    total = None
                    for d in range(cols):
                        one = lax.dot_general(
                            pieces[2 * d + e][entry, pl.ds(m * tile, tile), :],
                            weights[d][pl.ds(at, wide), :],
                            last_with_last,
                            preferred_element_type=F32,
                        )
                        total = one if total is None else total + one
                    out[pl.ds(e * half + m * tile, tile), pl.ds(at, wide)] = total
            return carry

        lax.fori_loop(0, mine // wide, body, 0)


def input_terms(pieces, weights, entry):
    cols, chunks = len(weights[0]), len(weights)
    half, width = pieces[0, 0].shape[1:]
    mine = weights[0][0].shape[0]
    call = pl.pallas_call(
        functools.partial(terms_kernel, cols),
        in_specs=[pl.BlockSpec(memory_space=pltpu.SMEM)] + in_vmem((2 + chunks) * cols),
        out_specs=tuple(in_vmem(chunks)),
        out_shape=(jax.ShapeDtypeStruct((2 * half, mine), F32),) * chunks,
        compiler_params=pltpu.CompilerParams(vmem_limit_bytes=GRANT),
        cost_estimate=pl.CostEstimate(
            flops=4 * half * mine * cols * width * chunks,
            bytes_accessed=2 * (4 * half + mine * chunks) * cols * width + 8 * half * mine * chunks,
            transcendentals=0,
        ),
    )
    operands = [pieces[d, e] for d in range(cols) for e in range(2)]
    operands += [w for chunk in weights for w in chunk]
    return list(call(entry.astype(jnp.int32).reshape(1), *operands))


def reduce_line(near, far, weights, starts, rows):
    z = lax.axis_index("row")
    chunks = range(len(weights))
    zero, one = jnp.zeros((), jnp.int32), jnp.ones((), jnp.int32)
    lower = jnp.where(z < 2, zero, one)
    at_end = jnp.where((z == 0) | (z == 3), one, zero).reshape(1)
    outer = [input_terms(near, [weights[c]], lower)[0] for c in chunks]
    came = [lax.ppermute(pack([outer[c]]), "row", [(0, 1), (3, 2)]) for c in chunks]
    message = pack(input_terms(far, weights, zero), came)
    from_end = lax.ppermute(message, "row", [(0, 1), (3, 2)])
    from_middle = lax.ppermute(message, "row", [(1, 2), (2, 1)])
    inward = pack(input_terms(near, weights, 1 - lower), [from_end])
    first = lax.ppermute(inward, "row", [(1, 2), (2, 1)])
    mixed = pack(outer, [from_middle], at_end, inward)
    other = lax.ppermute(mixed, "row", [(0, 1), (3, 2), (1, 0), (2, 3)])
    own = input_terms(far, weights, one)
    half = len(starts) // 2
    across = finish(own, first, other, starts[half:], rows)
    return finish(own, first, other, starts[:half], rows) + across


def spread_grad(grad, groups, rows, cols):
    z, y = lax.axis_index("row"), lax.axis_index("depth")
    half = grad.shape[0] // 2
    per = rows // 2
    width = grad.shape[1] // per
    other = lax.dynamic_slice_in_dim(grad, (1 - y) * half, half, 0)
    own = lax.dynamic_slice_in_dim(grad, y * half, half, 0)
    came = flip(other, "depth", 1, 2)

    def piece(j):
        to = lax.rem(z + j, rows)
        both = jnp.where(lax.div(to, per) == y, own, came)
        block = lax.dynamic_slice_in_dim(both, lax.rem(to, per) * width, width, 1)
        if not j:
            return block
        return lax.ppermute(block, "row", [(i, (i + j) % rows) for i in range(rows)])

    pieces = {j: piece(j) for group in groups for j in group}
    out = []
    bits = [1 << b for b in range(cols.bit_length() - 1)]
    for group in groups:
        have = {(0, 0): jnp.stack([pieces[j] for j in group])}
        for bit in reversed(bits[1:]):
            have.update({(d ^ bit, e): flip(v, "col", bit, cols) for (d, e), v in have.items()})
        have.update({(d, 1): flip(v, "depth", 1, 2) for (d, e), v in have.items()})
        for bit in bits[:1]:
            have.update({(d ^ bit, e): flip(v, "col", bit, cols) for (d, e), v in have.items()})
        out.append(have)
    return out


def per_device(rows, cols, tokens, weight, grad_output):
    q, y = lax.axis_index("col"), lax.axis_index("depth")
    features, outs = weight.shape
    mine = features // cols
    few = tokens.shape[0]
    block_rows = few * cols
    half = block_rows // 2
    part = mine // CHUNKS

    def token_piece(d):
        return lax.dynamic_slice_in_dim(tokens, (q ^ d) * mine, mine, 1)

    def row_start(d):
        return lax.rem((q ^ d) * few + y * half, block_rows)

    token_pieces = swap_pieces(token_piece, cols)
    block = jnp.concatenate([token_pieces[1]] * cols)
    for d, piece in enumerate(token_pieces):
        block = lax.dynamic_update_slice_in_dim(block, piece, row_start(d), 0)

    weights = []
    for h in range(CHUNKS):

        def weight_piece(d):
            return lax.dynamic_slice_in_dim(weight, (q ^ d) * mine + h * part, part, 0)

        weights.append(swap_pieces(weight_piece, cols))

    groups = [(1, 3), (2, 0)]
    spread = spread_grad(grad_output, groups, rows, cols)
    token_slots = gather_line(block, rows)

    starts = [row_start(d) for d in range(cols)]
    summed = reduce_line(spread[0], spread[1], weights, starts, few)

    grad_input = jnp.zeros((few, features), BF16)
    for d, piece in enumerate(swap_pieces(lambda d: summed[d], cols)):
        grad_input = lax.dynamic_update_slice_in_dim(grad_input, piece, (q ^ d) * mine, 1)

    all_tokens = jnp.concatenate(
        [token_slots[j][e * half : (e + 1) * half] for g in groups for e in range(2) for j in g]
    )

    def gradient_piece(d):
        piece = jnp.concatenate([spread[g][d, e].reshape(-1, outs) for g in range(2) for e in range(2)])
        return lax.dot_general(
            all_tokens, piece, first_with_first, preferred_element_type=F32
        ).astype(BF16)

    grad_weight = jnp.zeros((features, outs), BF16)
    for d, piece in enumerate(swap_pieces(gradient_piece, cols)):
        grad_weight = lax.dynamic_update_slice_in_dim(grad_weight, piece, (q ^ d) * mine, 0)
    return grad_input, grad_weight


def solution(mesh):
    rows, cols = mesh.shape["row"], mesh.shape["col"]

    def body(tokens, weight, grad_output):
        return per_device(rows, cols, tokens, weight, grad_output)

    return jax.shard_map(
        body,
        mesh=mesh,
        in_specs=(
            P(("row", "col"), "depth"),
            P("depth", ("col", "row")),
            P("row", ("col", "depth")),
        ),
        out_specs=(P(("row", "col"), "depth"), P("depth", ("col", "row"))),
        check_vma=False,
    )
```

```python
import functools

import jax
import jax.numpy as jnp
from jax import lax
from jax.experimental import pallas as pl
from jax.experimental.pallas import tpu as pltpu
from jax.sharding import PartitionSpec as P


BF16 = jnp.bfloat16
F32 = jnp.float32
last_with_last = (((1,), (1,)), ((), ()))
first_with_first = (((0,), (0,)), ((), ()))
PAD = 16
GRANT = 20 * 2**20
TILE = 64
LIFT = 7.5
CHUNKS = 1


def flip(value, axis, bit, size):
    return lax.ppermute(value, axis, [(i, i ^ bit) for i in range(size)])


def swap_pieces(piece_for, size):
    got = {d: flip(piece_for(d), "col", d, size) for d in sorted(range(1, size), reverse=True)}
    got[0] = piece_for(0)
    return [got[d] for d in range(size)]


def gather_line(mine, size):
    up, down = [mine], [mine]
    for s in range(1, size):
        up.append(lax.ppermute(up[-1], "row", [(i, i + 1) for i in range(s - 1, size - 1)]))
        down.append(lax.ppermute(down[-1], "row", [(i, i - 1) for i in range(1, size - s + 1)]))
    z = lax.axis_index("row")
    ends = jnp.where(z == 0, down[3], up[3])
    outer = jnp.where((z == 0) | (z == 3), ends, jnp.where(z == 1, up[1], down[1]))
    opposite = jnp.where(z < 2, down[2], up[2])
    inner = jnp.where(z < 2, down[1], up[1])
    return outer, opposite, inner, mine


def unpacked(ref, rows, cols):
    scale = ref[pl.ds(ref.shape[0] - PAD, 8), cols].astype(F32)[:1] - LIFT
    coded = ref[rows, cols].astype(F32)
    size = jnp.exp2(jnp.log2(jnp.abs(coded)) * 0.0625 + scale)
    return jnp.where(coded < 0, -size, size)


def parts_of(terms, came):
    at = 0
    for i, term in enumerate(terms):
        width = term.shape[1]
        mine = pl.ds(at, width)
        if not came:
            yield mine, term, None, None
        elif len(came) == len(terms):
            yield mine, term, came[i], pl.ds(0, width)
        else:
            yield mine, term, came[0], mine
        at += width


def encode(terms, came, out, total):
    size, width = total.shape

    def add(t, tops):
        rows = pl.ds(pl.multiple_of(t * TILE, TILE), TILE)
        after = []
        for top, (mine, term, message, cols) in zip(tops, parts_of(terms, came)):
            value = term[rows, :]
            if message is not None:
                value = value + unpacked(message, rows, cols)
            total[rows, mine] = value
            after.append(jnp.maximum(top, jnp.max(jnp.abs(value), axis=0, keepdims=True)))
        return tuple(after)

    low = tuple(jnp.full((1, term.shape[1]), 1e-30, F32) for term in terms)
    tops = lax.fori_loop(0, size // TILE, add, low)
    top = functools.reduce(jnp.maximum, [jnp.max(t, axis=1, keepdims=True) for t in tops])
    power = jnp.floor(jnp.log2(top)) + 1.0
    scale = jnp.exp2(LIFT - power)

    def code(t, carry):
        rows = pl.ds(pl.multiple_of(t * TILE, TILE), TILE)
        value = total[rows, :]
        unit = value * scale
        unit = unit * unit
        unit = unit * unit
        unit = unit * unit
        unit = unit * unit
        out[rows, :] = jnp.where(value < 0, -unit, unit).astype(BF16)
        return carry

    lax.fori_loop(0, size // TILE, code, 0)
    out[pl.ds(size, PAD), :] = jnp.broadcast_to(power, (PAD, width)).astype(BF16)


def pack_kernel(count, at_end, *refs):
    refs = list(refs)
    total, out = refs.pop(), refs.pop()
    terms, came = refs[:count], refs[count:]
    if at_end is None:
        encode(terms, came, out, total)
        return
    other = came.pop()

    @pl.when(at_end[0] == 1)
    def _():
        out[...] = other[...]

    @pl.when(at_end[0] != 1)
    def _():
        encode(terms, came, out, total)


def in_vmem(count):
    return [pl.BlockSpec(memory_space=pltpu.VMEM)] * count


def pack(terms, came=(), at_end=None, other=None):
    size, width = terms[0].shape[0], sum(term.shape[1] for term in terms)
    operands = [*terms, *came]
    specs = in_vmem(len(operands))
    kernel = functools.partial(pack_kernel, len(terms), None)
    if other is not None:
        operands = [at_end, *operands, other]
        specs = [pl.BlockSpec(memory_space=pltpu.SMEM)] + specs + in_vmem(1)
        kernel = functools.partial(pack_kernel, len(terms))
    return pl.pallas_call(
        kernel,
        in_specs=specs,
        out_specs=in_vmem(1)[0],
        out_shape=jax.ShapeDtypeStruct((size + PAD, width), BF16),
        scratch_shapes=[pltpu.VMEM((size, width), F32)],
        compiler_params=pltpu.CompilerParams(vmem_limit_bytes=GRANT),
        cost_estimate=pl.CostEstimate(
            flops=size * width * 4000, bytes_accessed=size * width * 8, transcendentals=0
        ),
    )(*operands)


def finish_kernel(count, starts, *refs):
    terms, (one, two), outs = refs[:count], refs[count : count + 2], refs[count + 2 :]
    tile = min(TILE, outs[0].shape[0])
    for i, out in enumerate(outs):
        for t in range(out.shape[0] // tile):
            rows = pl.ds(pl.multiple_of(starts[i] + t * tile, tile), tile)
            for mine, term, message, cols in parts_of(terms, [one]):
                value = term[rows, :] + unpacked(one, rows, cols) + unpacked(two, rows, cols)
                out[pl.ds(t * tile, tile), mine] = value.astype(BF16)


def finish(terms, one, two, starts, rows):
    width, count = one.shape[1], len(terms)
    call = pl.pallas_call(
        functools.partial(finish_kernel, count),
        in_specs=[pl.BlockSpec(memory_space=pltpu.SMEM)] + in_vmem(count + 2),
        out_specs=tuple(in_vmem(len(starts))),
        out_shape=(jax.ShapeDtypeStruct((rows, width), BF16),) * len(starts),
        compiler_params=pltpu.CompilerParams(vmem_limit_bytes=GRANT),
        cost_estimate=pl.CostEstimate(
            flops=rows * len(starts) * width * 4000,
            bytes_accessed=rows * len(starts) * width * 10,
            transcendentals=0,
        ),
    )
    return list(call(jnp.stack(starts).astype(jnp.int32), *terms, one, two))


def terms_kernel(cols, which, *refs):
    pieces, refs = refs[: 2 * cols], refs[2 * cols :]
    chunks = len(refs) // (cols + 1)
    half = pieces[0].shape[1]
    entry = which[0]
    tile = min(half, 256)
    for c in range(chunks):
        weights, out = refs[c * cols : (c + 1) * cols], refs[chunks * cols + c]
        mine = weights[0].shape[0]
        wide = min(mine, 256)

        def body(n, carry):
            at = pl.multiple_of(n * wide, wide)
            for e in range(2):
                for m in range(half // tile):
                    total = None
                    for d in range(cols):
                        one = lax.dot_general(
                            pieces[2 * d + e][entry, pl.ds(m * tile, tile), :],
                            weights[d][pl.ds(at, wide), :],
                            last_with_last,
                            preferred_element_type=F32,
                        )
                        total = one if total is None else total + one
                    out[pl.ds(e * half + m * tile, tile), pl.ds(at, wide)] = total
            return carry

        lax.fori_loop(0, mine // wide, body, 0)


def input_terms(pieces, weights, entry):
    cols, chunks = len(weights[0]), len(weights)
    half, width = pieces[0, 0].shape[1:]
    mine = weights[0][0].shape[0]
    call = pl.pallas_call(
        functools.partial(terms_kernel, cols),
        in_specs=[pl.BlockSpec(memory_space=pltpu.SMEM)] + in_vmem((2 + chunks) * cols),
        out_specs=tuple(in_vmem(chunks)),
        out_shape=(jax.ShapeDtypeStruct((2 * half, mine), F32),) * chunks,
        compiler_params=pltpu.CompilerParams(vmem_limit_bytes=GRANT),
        cost_estimate=pl.CostEstimate(
            flops=4 * half * mine * cols * width * chunks,
            bytes_accessed=2 * (4 * half + mine * chunks) * cols * width + 8 * half * mine * chunks,
            transcendentals=0,
        ),
    )
    operands = [pieces[d, e] for d in range(cols) for e in range(2)]
    operands += [w for chunk in weights for w in chunk]
    return list(call(entry.astype(jnp.int32).reshape(1), *operands))


def reduce_line(outers, opposites, inners, weights, starts, rows):
    z = lax.axis_index("row")
    chunks = range(len(weights))
    zero, one = jnp.zeros((), jnp.int32), jnp.ones((), jnp.int32)
    at_end = jnp.where((z == 0) | (z == 3), one, zero).reshape(1)
    outer = [input_terms(outers, [weights[c]], zero)[0] for c in chunks]
    came = [lax.ppermute(pack([outer[c]]), "row", [(0, 1), (3, 2)]) for c in chunks]
    message = pack(input_terms(opposites, weights, zero), came)
    from_end = lax.ppermute(message, "row", [(0, 1), (3, 2)])
    from_middle = lax.ppermute(message, "row", [(1, 2), (2, 1)])
    inward = pack(input_terms(inners, weights, zero), [from_end])
    first = lax.ppermute(inward, "row", [(1, 2), (2, 1)])
    mixed = pack(outer, [from_middle], at_end, inward)
    other = lax.ppermute(mixed, "row", [(0, 1), (3, 2), (1, 0), (2, 3)])
    own = input_terms(inners, weights, one)
    half = len(starts) // 2
    across = finish(own, first, other, starts[half:], rows)
    return finish(own, first, other, starts[:half], rows) + across


def spread_grad(grad, rows, cols):
    z, y = lax.axis_index("row"), lax.axis_index("depth")
    half = grad.shape[0] // 2
    per = rows // 2
    width = grad.shape[1] // per
    other = lax.dynamic_slice_in_dim(grad, (1 - y) * half, half, 0)
    own = lax.dynamic_slice_in_dim(grad, y * half, half, 0)
    came = flip(other, "depth", 1, 2)

    def piece(j):
        to = lax.rem(z + j, rows)
        both = jnp.where(lax.div(to, per) == y, own, came)
        block = lax.dynamic_slice_in_dim(both, lax.rem(to, per) * width, width, 1)
        if not j:
            return block
        return lax.ppermute(block, "row", [(i, (i + j) % rows) for i in range(rows)])

    one, three, two, own_rows = piece(1), piece(3), piece(2), piece(0)
    groups = [
        [jnp.where(z < 2, one, three)],
        [two],
        [jnp.where(z < 2, three, one), own_rows],
    ]
    out = []
    bits = [1 << b for b in range(cols.bit_length() - 1)]
    for group in groups:
        have = {(0, 0): jnp.stack(group)}
        for bit in reversed(bits[1:]):
            have.update({(d ^ bit, e): flip(v, "col", bit, cols) for (d, e), v in have.items()})
        have.update({(d, 1): flip(v, "depth", 1, 2) for (d, e), v in have.items()})
        for bit in bits[:1]:
            have.update({(d ^ bit, e): flip(v, "col", bit, cols) for (d, e), v in have.items()})
        out.append(have)
    return out


def per_device(rows, cols, tokens, weight, grad_output):
    q, y = lax.axis_index("col"), lax.axis_index("depth")
    features, outs = weight.shape
    mine = features // cols
    few = tokens.shape[0]
    block_rows = few * cols
    half = block_rows // 2
    part = mine // CHUNKS

    def token_piece(d):
        return lax.dynamic_slice_in_dim(tokens, (q ^ d) * mine, mine, 1)

    def row_start(d):
        return lax.rem((q ^ d) * few + y * half, block_rows)

    token_pieces = swap_pieces(token_piece, cols)
    block = jnp.concatenate([token_pieces[1]] * cols)
    for d, piece in enumerate(token_pieces):
        block = lax.dynamic_update_slice_in_dim(block, piece, row_start(d), 0)

    weights = []
    for h in range(CHUNKS):

        def weight_piece(d):
            return lax.dynamic_slice_in_dim(weight, (q ^ d) * mine + h * part, part, 0)

        weights.append(swap_pieces(weight_piece, cols))

    spread = spread_grad(grad_output, rows, cols)
    outer, opposite, inner, own = gather_line(block, rows)

    starts = [row_start(d) for d in range(cols)]
    summed = reduce_line(*spread, weights, starts, few)

    grad_input = jnp.zeros((few, features), BF16)
    for d, piece in enumerate(swap_pieces(lambda d: summed[d], cols)):
        grad_input = lax.dynamic_update_slice_in_dim(grad_input, piece, (q ^ d) * mine, 1)

    groups = [outer], [opposite], [inner, own]
    all_tokens = jnp.concatenate(
        [t[e * half : (e + 1) * half] for group in groups for e in range(2) for t in group]
    )

    def gradient_piece(d):
        piece = jnp.concatenate([spread[g][d, e].reshape(-1, outs) for g in range(3) for e in range(2)])
        return lax.dot_general(
            all_tokens, piece, first_with_first, preferred_element_type=F32
        ).astype(BF16)

    grad_weight = jnp.zeros((features, outs), BF16)
    for d, piece in enumerate(swap_pieces(gradient_piece, cols)):
        grad_weight = lax.dynamic_update_slice_in_dim(grad_weight, piece, (q ^ d) * mine, 0)
    return grad_input, grad_weight


def solution(mesh):
    rows, cols = mesh.shape["row"], mesh.shape["col"]

    def body(tokens, weight, grad_output):
        return per_device(rows, cols, tokens, weight, grad_output)

    return jax.shard_map(
        body,
        mesh=mesh,
        in_specs=(
            P(("row", "col"), "depth"),
            P("depth", ("col", "row")),
            P("row", ("col", "depth")),
        ),
        out_specs=(P(("row", "col"), "depth"), P("depth", ("col", "row"))),
        check_vma=False,
    )
```
